32 devices in a mesh: kgrp: 2 (over y), band: 4 (over z), fft: 4 (over x, core).
Axes of the slice: x: 2, y: 2, z: 4, core: 2. Of those that a mesh axis runs over, the one named last changes fastest.
Arguments:
- orbitals: float32 [8, 64, 64, 128], P(('kgrp', 'band'), 'fft'), parts along dimension 0, may hold values from -6 to 6
- partners: float32 [8, 64, 64, 128], P(('kgrp', 'band'), 'fft'), parts along dimension 0, may hold values from -6 to 6
- shift_table: float32 [8, 3], replicated, may hold values from -0.5 to 0.5
- shift_index: int32 [8], P('kgrp'), parts along dimension 0, may hold values from 0 to 7
Outputs:
- potential: float32 [8, 64, 64, 128], P(('kgrp', 'band'), 'fft'), parts along dimension 0
- projector: float32 [8, 64, 64, 128], P(('kgrp', 'band'), 'fft'), parts along dimension 0
The draws below stay inside these ranges and needn't reach their ends.
There are 2 independent parts, one for each index of `kgrp`. The reference program is written for one: setup_inputs(seed, part) draws one part's arguments, and reference() takes and returns one part's arrays. A program takes and returns all parts, laid end to end along the dimension named above; an argument that names none is the same for every part. Nothing has to cross between parts.
All inputs are finite; a program needn't handle non-finite values.
Results may differ from the reference program's by a relative error of at most 0.0001.
Values sent between devices are 32-bit elements; how exact they have to be, the bound alone decides.
No kernel may reach another device: no remote copies, remote signals or barrier semaphores. Data moves between devices by JAX's collectives and lax.ppermute only.
A program may use at most 64 MiB of HBM per device.

```python
import math
import jax
import jax.numpy as jnp
from jax import lax

GRID = 64
NQ = 8
BANDS = 4
PARTNERS = 4


def touch_ends(drawn, rng, least, top_value):
    longest = drawn.shape.index(max(drawn.shape))
    spots = []
    for shift in (0, 1):
        where = [jax.random.randint(jax.random.fold_in(rng, axis), (), 0, length) for axis, length in enumerate(drawn.shape)]
        where[longest] = (where[longest] + shift) % drawn.shape[longest]
        spots.append(tuple(where))
    return drawn.at[spots[0]].set(least).at[spots[1]].set(top_value)


def block_levels(stream_key, dims, pieces, low, high):
    loudness = 1.0
    for dim, parts in pieces:
        heights = jax.random.uniform(jax.random.fold_in(jax.random.fold_in(stream_key, 6), dim), (parts,), jnp.float32, low / len(pieces), high / len(pieces))
        loudness = loudness * jnp.repeat(jnp.exp(heights), dims[dim] // parts).reshape((-1,) + (1,) * (len(dims) - 1 - dim))
    return loudness


def noise(stream_key, shape, scale, bound, split=(), kind=jnp.bfloat16):
    result = jax.random.normal(stream_key, shape, jnp.float32) * scale
    if len(split) > 0:
        result = block_levels(stream_key, shape, split, -0.22, 0.18) * result
    return jnp.clip(result, min=-bound, max=bound).astype(kind)


def setup_inputs(seed: int = 0, part: int = 0) -> dict:
    arg_keys = jax.random.split(jax.random.key(seed), 5)
    part_keys = jax.random.split(jax.random.fold_in(arg_keys[4], part), 5)
    orbitals = noise(part_keys[0], (BANDS, GRID, GRID, 2 * GRID), 0.7, 6.0, ((0, 4), (1, 4)), jnp.float32)
    partners = noise(part_keys[1], (PARTNERS, GRID, GRID, 2 * GRID), 0.7, 6.0, ((0, 4), (1, 4)), jnp.float32)
    shift_table = jnp.clip(jax.random.uniform(arg_keys[2], (NQ, 3), jnp.float32, -0.5, 0.5), -0.5, 0.5)
    shift_index = touch_ends(jax.random.randint(part_keys[3], (PARTNERS,), 0, NQ), jax.random.fold_in(part_keys[3], 1), 0, NQ - 1).astype(jnp.int32)
    return {"orbitals": orbitals, "partners": partners, "shift_table": shift_table, "shift_index": shift_index}


HIGHEST = lax.Precision.HIGHEST
SCREEN_SQUARE = 0.25
FOUR_PI = 4.0 * math.pi

def frequency(positions, extent):
    return jnp.where(positions < extent // 2, positions, positions - extent).astype(jnp.float32)

def rotate(field):
    extent = field.shape[-1] // 2
    return jnp.concatenate([field[..., extent:], -field[..., :extent]], axis=-1)

def factor_inverse(over_real, over_imag):
    matrix_order = over_real.shape[0]
    positions = jnp.arange(matrix_order, dtype=jnp.int32)
    zero_start = jnp.zeros_like(over_real)

    def chol_step(column, lowers):
        lower_real, lower_imag = lowers
        row_real = lower_real[column]
        row_imag = lower_imag[column]
        resid_real = over_real[:, column] - (jnp.dot(lower_real, row_real, precision=HIGHEST) + jnp.dot(lower_imag, row_imag, precision=HIGHEST))
        resid_imag = over_imag[:, column] - (jnp.dot(lower_imag, row_real, precision=HIGHEST) - jnp.dot(lower_real, row_imag, precision=HIGHEST))
        pivot_value = jnp.sqrt(resid_real[column])
        below_diag = positions > column
        at_diag = positions == column
        new_real = jnp.where(below_diag, resid_real / pivot_value, jnp.where(at_diag, pivot_value, 0.0))
        new_imag = jnp.where(below_diag, resid_imag / pivot_value, 0.0)
        chosen = positions[None, :] == column
        return (jnp.where(chosen, new_real[:, None], lower_real), jnp.where(chosen, new_imag[:, None], lower_imag))
    lower_real, lower_imag = lax.fori_loop(0, matrix_order, chol_step, (zero_start, zero_start))

    def solve_step(row_index, inverses):
        inv_real, inv_imag = inverses
        row_real = lower_real[row_index]
        row_imag = lower_imag[row_index]
        sum_real = jnp.dot(row_real, inv_real, precision=HIGHEST) - jnp.dot(row_imag, inv_imag, precision=HIGHEST)
        sum_imag = jnp.dot(row_real, inv_imag, precision=HIGHEST) + jnp.dot(row_imag, inv_real, precision=HIGHEST)
        unit_row = (positions == row_index).astype(over_real.dtype)
        pivot_value = lower_real[row_index, row_index]
        new_real = (unit_row - sum_real) / pivot_value
        new_imag = -sum_imag / pivot_value
        chosen = positions[:, None] == row_index
        return (jnp.where(chosen, new_real[None, :], inv_real), jnp.where(chosen, new_imag[None, :], inv_imag))
    return lax.fori_loop(0, matrix_order, solve_step, (zero_start, zero_start))

def reference(orbitals, partners, shift_table, shift_index):
    extent = orbitals.shape[1]
    orbital_field = orbitals[..., :extent] + 1j * orbitals[..., extent:]
    partner_field = partners[..., :extent] + 1j * partners[..., extent:]
    grid_freq = frequency(jnp.arange(extent, dtype=jnp.int32), extent).astype(orbitals.dtype)

    def partner_term(running, member):
        single, chosen_index = member
        qvector = shift_table[chosen_index]
        denominator = (grid_freq[:, None, None] + qvector[0]) ** 2 + (grid_freq[None, :, None] + qvector[1]) ** 2 + (grid_freq[None, None, :] + qvector[2]) ** 2 + SCREEN_SQUARE
        kernel = FOUR_PI / denominator
        density = jnp.conj(single)[None] * orbital_field
        field = jnp.fft.ifftn(jnp.fft.fftn(density, axes=(1, 2, 3)) * kernel[None], axes=(1, 2, 3))
        return (running + single[None] * field, None)
    start_field = jnp.zeros(orbital_field.shape, orbital_field.dtype)
    exchange_field, _ = lax.scan(partner_term, start_field, (partner_field, shift_index))
    potential = jnp.concatenate([exchange_field.real, exchange_field.imag], axis=-1).astype(orbitals.dtype)
    total_bands = potential.shape[0]
    turned = rotate(potential)
    flat_orbitals = orbitals.reshape(total_bands, -1)
    flat_pot = potential.reshape(total_bands, -1)
    flat_turned = turned.reshape(total_bands, -1)
    volume = float(extent ** 3)
    over_real = jnp.einsum('ik,jk->ij', flat_orbitals, flat_pot, precision=HIGHEST) / volume
    over_imag = jnp.einsum('ik,jk->ij', flat_orbitals, flat_turned, precision=HIGHEST) / volume
    inv_real, inv_imag = factor_inverse(over_real, over_imag)
    projector = jnp.dot(inv_real, flat_pot, precision=HIGHEST) + jnp.dot(inv_imag, flat_turned, precision=HIGHEST)
    return (potential, projector.reshape(potential.shape))
```

```python
import math

import jax
import jax.numpy as jnp
from jax import lax
from jax.experimental import pallas as pl
from jax.experimental.pallas import tpu as pltpu
from jax.sharding import PartitionSpec as P

PREC = lax.Precision.HIGH
SCREEN_SQUARE = 0.25
FOUR_PI = 4.0 * math.pi
GROUPS = 2


def angle_pair(extent, sign):
    positions = jnp.arange(extent, dtype=jnp.int32)
    product = positions[:, None] * positions[None, :] % extent
    angle = 2.0 * math.pi / extent * product.astype(jnp.float32)
    return (jnp.cos(angle), sign * jnp.sin(angle))


def last_table(extent, sign):
    cosine, sine = angle_pair(extent, sign)
    upper = jnp.concatenate([cosine, sine], axis=1)
    lower = jnp.concatenate([-sine, cosine], axis=1)
    return jnp.concatenate([upper, lower], axis=0)


def middle_table(extent, sign):
    cosine, sine = angle_pair(extent, sign)
    return jnp.stack([jnp.stack([cosine, -sine], -1), jnp.stack([sine, cosine], -1)], 1)


def along_last(field, table):
    shape = field.shape
    flat = field.reshape(-1, shape[-1])
    return jnp.dot(flat, table, precision=PREC).reshape(shape)


def along_axis(field, table, axis_number):
    shape = field.shape
    extent = shape[-1] // 2
    split = field.reshape(shape[0], shape[1], shape[2], 2, extent)
    if axis_number == 1:
        result = jnp.einsum("kcnd,pnbdz->pkbcz", table, split, precision=PREC)
    else:
        result = jnp.einsum("kcnd,pandz->pakcz", table, split, precision=PREC)
    return result.reshape(shape)


def times_conj(left, right):
    extent = left.shape[-1] // 2
    left_real, left_imag = (left[..., :extent], left[..., extent:])
    right_real, right_imag = (right[..., :extent], right[..., extent:])
    return jnp.concatenate(
        [
            left_real * right_real + left_imag * right_imag,
            left_real * right_imag - left_imag * right_real,
        ],
        axis=-1,
    )


def times(left, right):
    extent = left.shape[-1] // 2
    left_real, left_imag = (left[..., :extent], left[..., extent:])
    right_real, right_imag = (right[..., :extent], right[..., extent:])
    return jnp.concatenate(
        [
            left_real * right_real - left_imag * right_imag,
            left_real * right_imag + left_imag * right_real,
        ],
        axis=-1,
    )


def rotate(field):
    extent = field.shape[-1] // 2
    return jnp.concatenate([field[..., extent:], -field[..., :extent]], axis=-1)


def frequency(positions, extent):
    return jnp.where(positions < extent // 2, positions, positions - extent).astype(jnp.float32)


def kernel_block(qvectors, y_start, y_count, extent):
    first_freq = frequency(jnp.arange(extent, dtype=jnp.int32), extent)
    second_freq = frequency(y_start + jnp.arange(y_count, dtype=jnp.int32), extent)
    third_freq = frequency(jnp.arange(2 * extent, dtype=jnp.int32) % extent, extent)
    first_part = (first_freq[None, :] + qvectors[:, 0:1]) ** 2
    second_part = (second_freq[None, :] + qvectors[:, 1:2]) ** 2
    third_part = (third_freq[None, :] + qvectors[:, 2:3]) ** 2
    denominator = (
        first_part[:, :, None, None]
        + second_part[:, None, :, None]
        + third_part[:, None, None, :]
        + SCREEN_SQUARE
    )
    return FOUR_PI / extent**3 / denominator


def factor_kernel(over_ref, inv_ref, *, order, scale):
    total = jnp.sum(over_ref[...], axis=0) * scale
    size = total.shape[-1]
    res_real, res_imag = total[0], total[1]
    rows = lax.broadcasted_iota(jnp.int32, (size, size), 0)
    cols = lax.broadcasted_iota(jnp.int32, (size, size), 1)
    same = rows == cols
    inv_real = jnp.where(same, 1.0, 0.0).astype(jnp.float32)
    inv_imag = jnp.zeros_like(inv_real)
    across = lambda v: jnp.sum(v, axis=1, keepdims=True)
    down = lambda v: jnp.sum(v, axis=0, keepdims=True)
    for step in range(order):
        at_col = cols == step
        pivot = down(across(jnp.where(at_col & (rows == step), res_real, 0.0)))
        root = 1.0 / jnp.sqrt(pivot)
        below = at_col & (rows > step)
        col_real = across(jnp.where(below, res_real, 0.0)) * root
        col_imag = across(jnp.where(below, res_imag, 0.0)) * root
        row_real = down(jnp.where(same, col_real, 0.0))
        row_imag = down(jnp.where(same, col_imag, 0.0))
        res_real = res_real - (col_real * row_real + col_imag * row_imag)
        res_imag = res_imag - (col_imag * row_real - col_real * row_imag)
        at_row = rows == step
        inv_real = jnp.where(at_row, inv_real * root, inv_real)
        inv_imag = jnp.where(at_row, inv_imag * root, inv_imag)
        lead_real = down(jnp.where(at_row, inv_real, 0.0))
        lead_imag = down(jnp.where(at_row, inv_imag, 0.0))
        inv_real = inv_real - (col_real * lead_real - col_imag * lead_imag)
        inv_imag = inv_imag - (col_real * lead_imag + col_imag * lead_real)
    inv_ref[0] = inv_real
    inv_ref[1] = inv_imag


def factor_inverse(pieces, order, scale):
    size = pieces.shape[-1]
    body = lambda a, b: factor_kernel(a, b, order=order, scale=scale)
    return pl.pallas_call(
        body, out_shape=jax.ShapeDtypeStruct((2, size, size), jnp.float32), name="factor"
    )(pieces)


def ring_shift(value, axis_name, count, step):
    return lax.ppermute(value, axis_name, [(i, (i + step) % count) for i in range(count)])


def gather_small(value, axis_name, count):
    copies = jnp.broadcast_to(value[None], (count,) + value.shape)
    return lax.all_to_all(copies, axis_name, split_axis=0, concat_axis=0, tiled=True)


def exchange_body(band_size, fft_size, orbitals, partners, shift_table, shift_index):
    extent = orbitals.shape[2]
    band_count, slab = orbitals.shape[:2]
    partner_count = partners.shape[0]
    y_count = extent // fft_size
    my_band = lax.axis_index("band")
    y_start = lax.axis_index("fft") * y_count
    forward_last, inverse_last = last_table(extent, -1.0), last_table(extent, 1.0)
    forward_mid, inverse_mid = middle_table(extent, -1.0), middle_table(extent, 1.0)

    arrived = [partners] + [
        ring_shift(partners, "band", band_size, step) for step in range(1, band_size)
    ]
    per_group = -(-band_size // GROUPS)
    potential = 0.0
    for first in range(0, band_size, per_group):
        steps = list(range(first, min(first + per_group, band_size)))
        block = jnp.concatenate([arrived[step] for step in steps], axis=0)
        ids = jnp.concatenate(
            [
                (my_band - step) % band_size * partner_count + jnp.arange(partner_count)
                for step in steps
            ]
        )
        qvectors = shift_table[shift_index[ids]]
        kernel = kernel_block(qvectors, y_start, y_count, extent)
        density = times_conj(block[None], orbitals[:, None])
        shape = density.shape
        flat = density.reshape((-1,) + shape[2:])
        spectrum = along_axis(along_last(flat, forward_last), forward_mid, 2)
        spectrum = lax.all_to_all(spectrum, "fft", split_axis=2, concat_axis=1, tiled=True)
        spectrum = along_axis(spectrum, forward_mid, 1)
        spectrum = spectrum.reshape((band_count, -1) + spectrum.shape[1:]) * kernel[None]
        spectrum = along_axis(spectrum.reshape((-1,) + spectrum.shape[2:]), inverse_mid, 1)
        spectrum = lax.all_to_all(spectrum, "fft", split_axis=1, concat_axis=2, tiled=True)
        field = along_last(along_axis(spectrum, inverse_mid, 2), inverse_last).reshape(shape)
        potential = potential + jnp.sum(times(block[None], field), axis=1)

    def spread(value):
        rows = value.reshape(band_count, -1, 2 * extent)
        return lax.all_to_all(rows, "band", split_axis=1, concat_axis=0, tiled=True)

    sub_orbitals = spread(orbitals)
    sub_pot = spread(potential)
    total_bands = sub_pot.shape[0]
    sub_turned = rotate(sub_pot)
    flat_pot = sub_pot.reshape(total_bands, -1)
    flat_turned = sub_turned.reshape(total_bands, -1)
    both = jnp.stack([flat_pot, flat_turned])
    over = jnp.einsum("ik,cjk->cij", sub_orbitals.reshape(total_bands, -1), both, precision=PREC)
    size = max(8, total_bands)
    over = jnp.pad(over, ((0, 0), (0, size - total_bands), (0, size - total_bands)))
    pieces = gather_small(over, ("band", "fft"), band_size * fft_size)
    inverse = factor_inverse(pieces, total_bands, 1.0 / float(extent**3))
    inverse = inverse[:, :total_bands, :total_bands]
    projector = jnp.einsum("clm,cmk->lk", inverse, both, precision=PREC)
    projector = projector.reshape(sub_pot.shape)
    projector = lax.all_to_all(projector, "band", split_axis=0, concat_axis=1, tiled=True)
    return (potential, projector.reshape(orbitals.shape))


def solution(mesh):
    spec = P(("kgrp", "band"), "fft", None, None)
    band_size, fft_size = mesh.shape["band"], mesh.shape["fft"]
    body = lambda *arrays: exchange_body(band_size, fft_size, *arrays)
    return jax.shard_map(
        body,
        mesh=mesh,
        in_specs=(spec, spec, P(), P("kgrp")),
        out_specs=(spec, spec),
        check_vma=False,
    )
```

```python
import math

import jax
import jax.numpy as jnp
import numpy as np
from jax import lax
from jax.experimental import pallas as pl
from jax.experimental.pallas import tpu as pltpu
from jax.sharding import PartitionSpec as P

PREC = lax.Precision.HIGH
SCREEN_SQUARE = 0.25
FOUR_PI = 4.0 * math.pi


def lane_table(extent, sign):
    index = np.arange(extent)
    wave = np.exp(sign * 2j * np.pi / extent * (np.outer(index, index) % extent))
    full = np.kron(np.array([[1.0, 1.0], [1.0, -1.0]]), wave)
    return np.block([[full.real, full.imag], [-full.imag, full.real]])


def row_table(half, sign):
    index = np.arange(half)
    wave = np.exp(sign * 2j * np.pi / half * (np.outer(index, index) % half))
    return np.block([[wave.real, -wave.imag], [wave.imag, wave.real]])


def twiddle_table(extent, sign):
    half = extent // 2
    wave = np.exp(sign * 2j * np.pi / extent * np.arange(half))
    wave = np.concatenate(
        [np.ones((half, extent)), np.broadcast_to(wave[:, None], (half, extent))], axis=1
    )
    return jnp.asarray(np.stack([wave.real, wave.imag]), jnp.float32)


def halves(table):
    table = np.asarray(table, np.float32)
    high = table.astype(jnp.bfloat16)
    low = (table - high.astype(np.float32)).astype(jnp.bfloat16)
    return high, low


def stage_tables(extent, sign):
    high, low = halves(lane_table(extent, sign))
    lanes = jnp.stack([jnp.asarray(high), jnp.asarray(low)])
    high, low = halves(row_table(extent // 2, sign))
    rows = jnp.asarray(np.concatenate([high, high, low], axis=1))
    return lanes, rows, twiddle_table(extent, sign)


def split_value(value):
    high = value.astype(jnp.bfloat16)
    low = (value - high.astype(jnp.float32)).astype(jnp.bfloat16)
    return high, low


def dot(left, right):
    return jnp.dot(left, right, preferred_element_type=jnp.float32)


def on_lanes(real, imag, table_ref):
    high, low = split_value(jnp.concatenate([real, imag], axis=1))
    out = dot(high, table_ref[0]) + (dot(low, table_ref[0]) + dot(high, table_ref[1]))
    lanes = real.shape[1]
    return out[:, :lanes], out[:, lanes:]


def on_rows(stacked, table_ref):
    high, low = split_value(stacked)
    return dot(table_ref[...], jnp.concatenate([high, low, high], axis=0))


def unpack(tile):
    half, extent = tile.shape[0] // 2, tile.shape[1] // 2
    top, bottom = tile[:half], tile[half:]
    first = lax.broadcasted_iota(jnp.int32, top.shape, 1) < extent
    real = jnp.where(first, top, pltpu.roll(bottom, extent, 1))
    imag = jnp.where(first, pltpu.roll(top, extent, 1), bottom)
    return real, imag


def pack(real, imag):
    extent = real.shape[1] // 2
    first = lax.broadcasted_iota(jnp.int32, real.shape, 1) < extent
    top = jnp.where(first, real, pltpu.roll(imag, extent, 1))
    bottom = jnp.where(first, pltpu.roll(real, extent, 1), imag)
    return top, bottom


def forward_kernel(orb_ref, part_ref, lanes_ref, rows_ref, twid_ref, out_ref):
    count, extent = orb_ref.shape[1], orb_ref.shape[2]
    half = extent // 2
    devices, share = out_ref.shape[0], out_ref.shape[5]
    reals, imags = [], []
    for x in range(count):
        orb_real, orb_imag = unpack(orb_ref[0, x])
        part_real, part_imag = unpack(part_ref[0, x])
        reals.append(part_real * orb_real + part_imag * orb_imag)
        imags.append(part_real * orb_imag - part_imag * orb_real)
    real, imag = on_lanes(jnp.concatenate(reals, 0), jnp.concatenate(imags, 0), lanes_ref)
    cosine, sine = twid_ref[0], twid_ref[1]
    for x in range(0, count, 2):
        pair = []
        for at in (x, x + 1):
            re, im = real[at * half : (at + 1) * half], imag[at * half : (at + 1) * half]
            pair.append(
                jnp.concatenate([re * cosine - im * sine, re * sine + im * cosine], axis=0)
            )
        done = on_rows(jnp.concatenate(pair, axis=1), rows_ref)
        for at in (0, 1):
            piece = done[:, at * 2 * extent : (at + 1) * 2 * extent]
            for device in range(devices):
                lo = device * share
                out_ref[device, 0, 0, 0, x + at] = piece[lo : lo + share]
                out_ref[device, 0, 0, 1, x + at] = piece[half + lo : half + lo + share]


def inverse_kernel(spec_ref, part_ref, *refs, chained):
    prior_ref = refs[0] if chained else None
    lanes_ref, rows_ref, twid_ref, out_ref = refs[-4:]
    count, extent = part_ref.shape[1], part_ref.shape[2]
    half = extent // 2
    devices = spec_ref.shape[0]
    cosine, sine = twid_ref[0], twid_ref[1]
    reals, imags = [], []
    for x in range(0, count, 2):
        stacked = jnp.concatenate(
            [
                jnp.concatenate(
                    [spec_ref[d, 0, 0, c, at] for c in (0, 1) for d in range(devices)], axis=0
                )
                for at in (x, x + 1)
            ],
            axis=1,
        )
        done = on_rows(stacked, rows_ref)
        for at in (0, 1):
            piece = done[:, at * 2 * extent : (at + 1) * 2 * extent]
            re, im = piece[:half], piece[half:]
            reals.append(re * cosine - im * sine)
            imags.append(re * sine + im * cosine)
    real, imag = on_lanes(jnp.concatenate(reals, 0), jnp.concatenate(imags, 0), lanes_ref)
    first = pl.program_id(2) == 0
    for x in range(count):
        re, im = real[x * half : (x + 1) * half], imag[x * half : (x + 1) * half]
        part_real, part_imag = unpack(part_ref[0, x])
        top, bottom = pack(part_real * re - part_imag * im, part_real * im + part_imag * re)
        value = jnp.concatenate([top, bottom], axis=0)
        before = prior_ref[0, x] if chained else jnp.zeros_like(value)
        out_ref[0, x] = value + jnp.where(first, before, out_ref[0, x])


def turn(real, imag, step, count, sign):
    step = step % count
    if step == 0:
        return real, imag
    if 4 * step == count:
        return (-imag, real) if sign > 0 else (imag, -real)
    if 2 * step == count:
        return -real, -imag
    if 4 * step == 3 * count:
        return (imag, -real) if sign > 0 else (-imag, real)
    angle = 2.0 * math.pi * step / count
    cosine, sine = math.cos(angle), sign * math.sin(angle)
    return real * cosine - imag * sine, real * sine + imag * cosine


def small_dft(values, sign):
    count = len(values)
    if count == 1:
        return values
    even, odd = small_dft(values[0::2], sign), small_dft(values[1::2], sign)
    low, high = [], []
    for step in range(count // 2):
        turned_real, turned_imag = turn(*odd[step], step, count, sign)
        low.append((even[step][0] + turned_real, even[step][1] + turned_imag))
        high.append((even[step][0] - turned_real, even[step][1] - turned_imag))
    return low + high


def long_dft(values, sign):
    count, first = len(values), 1
    while first * first < count:
        first *= 2
    second = count // first
    columns = []
    for offset in range(second):
        part = small_dft(values[offset::second], sign)
        columns.append([turn(*part[k], offset * k, count, sign) for k in range(first)])
    out = [None] * count
    for k in range(first):
        for block, value in enumerate(small_dft([column[k] for column in columns], sign)):
            out[k + first * block] = value
    return out


def middle_kernel(first_ref, plane_ref, spec_ref, out_ref):
    field = pl.program_id(1)
    devices, slab = spec_ref.shape[0], spec_ref.shape[4]
    extent = devices * slab
    plane = plane_ref[0]
    values = [
        (spec_ref[x // slab, 0, 0, 0, x % slab], spec_ref[x // slab, 0, 0, 1, x % slab])
        for x in range(extent)
    ]
    values = long_dft(values, -1.0)
    scale = FOUR_PI / extent**3
    scaled = []
    for x, (real, imag) in enumerate(values):
        kernel = scale / (first_ref[field, x] + plane)
        scaled.append((real * kernel, imag * kernel))
    for x, (real, imag) in enumerate(long_dft(scaled, 1.0)):
        out_ref[x // slab, 0, 0, 0, x % slab] = real
        out_ref[x // slab, 0, 0, 1, x % slab] = imag


def whole_block(array):
    return pl.BlockSpec(array.shape, lambda *_: (0,) * array.ndim)


def chunk_of(slab):
    return math.gcd(slab, 8)


def cost(flops, count):
    return pl.CostEstimate(flops=int(flops), bytes_accessed=int(count), transcendentals=0)


def forward_call(orbitals, block, tables, devices):
    bands, slab, extent, lanes = orbitals.shape
    fields, step = block.shape[0], chunk_of(orbitals.shape[1])
    share = extent // 2 // devices
    grid_block = (1, step, extent, lanes)
    return pl.pallas_call(
        forward_kernel,
        grid=(bands, fields, slab // step),
        in_specs=[
            pl.BlockSpec(grid_block, lambda i, j, x: (i, x, 0, 0)),
            pl.BlockSpec(grid_block, lambda i, j, x: (j, x, 0, 0)),
        ]
        + [whole_block(table) for table in tables],
        out_specs=pl.BlockSpec(
            (devices, 1, 1, 2, step, share, lanes), lambda i, j, x: (0, i, j, 0, x, 0, 0)
        ),
        out_shape=jax.ShapeDtypeStruct(
            (devices, bands, fields, 2, slab, share, lanes), jnp.float32
        ),
        cost_estimate=cost(bands * fields * 1e9, bands * fields * orbitals[0].size * 12),
        name="forward",
    )(orbitals, block, *tables)


def middle_call(first_part, plane, spectrum):
    devices, bands, fields, _, slab, share, lanes = spectrum.shape
    spec = pl.BlockSpec(
        (devices, 1, 1, 2, slab, share, lanes), lambda i, j: (0, i, j, 0, 0, 0, 0)
    )
    return pl.pallas_call(
        middle_kernel,
        grid=(bands, fields),
        in_specs=[
            pl.BlockSpec(memory_space=pltpu.SMEM),
            pl.BlockSpec((1, share, lanes), lambda i, j: (j, 0, 0)),
            spec,
        ],
        out_specs=spec,
        out_shape=jax.ShapeDtypeStruct(spectrum.shape, jnp.float32),
        cost_estimate=cost(bands * fields * 1e9, spectrum.size * 8),
        name="middle",
    )(first_part, plane, spectrum)


def inverse_call(spectrum, block, prior, tables):
    devices, bands, fields, _, slab, share, lanes = spectrum.shape
    extent, step = block.shape[2], chunk_of(slab)
    grid_block = (1, step, extent, lanes)
    by_band = pl.BlockSpec(grid_block, lambda i, x, j: (i, x, 0, 0))
    chained = prior is not None
    extra = [prior] if chained else []
    body = lambda *refs: inverse_kernel(*refs, chained=chained)
    return pl.pallas_call(
        body,
        grid=(bands, slab // step, fields),
        in_specs=[
            pl.BlockSpec(
                (devices, 1, 1, 2, step, share, lanes), lambda i, x, j: (0, i, j, 0, x, 0, 0)
            ),
            pl.BlockSpec(grid_block, lambda i, x, j: (j, x, 0, 0)),
        ]
        + [by_band] * len(extra)
        + [whole_block(table) for table in tables],
        out_specs=by_band,
        out_shape=jax.ShapeDtypeStruct((bands, slab, extent, lanes), jnp.float32),
        cost_estimate=cost(bands * fields * 1e9, bands * fields * block[0].size * 12),
        name="inverse",
    )(spectrum, block, *extra, *tables)


def rotate(field):
    extent = field.shape[-1] // 2
    return jnp.concatenate([field[..., extent:], -field[..., :extent]], axis=-1)


def frequency(positions, extent):
    return jnp.where(positions < extent // 2, positions, positions - extent).astype(jnp.float32)


def kernel_parts(qvectors, row_start, row_count, extent):
    index = jnp.arange(extent, dtype=jnp.int32)
    parity = jnp.arange(2, dtype=jnp.int32)
    ky = 2 * (row_start + jnp.arange(row_count, dtype=jnp.int32))[:, None] + parity
    first = (frequency(index, extent)[None, :] + qvectors[:, 0:1]) ** 2
    second = (frequency(ky, extent)[None] + qvectors[:, 1, None, None]) ** 2
    third = (frequency(index, extent)[None, :] + qvectors[:, 2:3]) ** 2
    plane = second[:, :, :, None] + third[:, None, None, :] + SCREEN_SQUARE
    return first, plane.reshape(qvectors.shape[0], row_count, 2 * extent)


def factor_kernel(over_ref, inv_ref, *, order, scale):
    total = jnp.sum(over_ref[...], axis=0) * scale
    size = total.shape[-1]
    res_real, res_imag = total[0], total[1]
    rows = lax.broadcasted_iota(jnp.int32, (size, size), 0)
    cols = lax.broadcasted_iota(jnp.int32, (size, size), 1)
    same = rows == cols
    inv_real = jnp.where(same, 1.0, 0.0).astype(jnp.float32)
    inv_imag = jnp.zeros_like(inv_real)
    across = lambda v: jnp.sum(v, axis=1, keepdims=True)
    down = lambda v: jnp.sum(v, axis=0, keepdims=True)
    for step in range(order):
        at_col = cols == step
        pivot = down(across(jnp.where(at_col & (rows == step), res_real, 0.0)))
        root = 1.0 / jnp.sqrt(pivot)
        below = at_col & (rows > step)
        col_real = across(jnp.where(below, res_real, 0.0)) * root
        col_imag = across(jnp.where(below, res_imag, 0.0)) * root
        row_real = down(jnp.where(same, col_real, 0.0))
        row_imag = down(jnp.where(same, col_imag, 0.0))
        res_real = res_real - (col_real * row_real + col_imag * row_imag)
        res_imag = res_imag - (col_imag * row_real - col_real * row_imag)
        at_row = rows == step
        inv_real = jnp.where(at_row, inv_real * root, inv_real)
        inv_imag = jnp.where(at_row, inv_imag * root, inv_imag)
        lead_real = down(jnp.where(at_row, inv_real, 0.0))
        lead_imag = down(jnp.where(at_row, inv_imag, 0.0))
        inv_real = inv_real - (col_real * lead_real - col_imag * lead_imag)
        inv_imag = inv_imag - (col_real * lead_imag + col_imag * lead_real)
    inv_ref[0] = inv_real
    inv_ref[1] = inv_imag


def factor_inverse(pieces, order, scale):
    size = pieces.shape[-1]
    body = lambda a, b: factor_kernel(a, b, order=order, scale=scale)
    return pl.pallas_call(
        body, out_shape=jax.ShapeDtypeStruct((2, size, size), jnp.float32), name="factor"
    )(pieces)


def ring_shift(value, axis_name, count, step):
    return lax.ppermute(value, axis_name, [(i, (i + step) % count) for i in range(count)])


def gather_small(value, axis_name, count):
    copies = jnp.broadcast_to(value[None], (count,) + value.shape)
    return lax.all_to_all(copies, axis_name, split_axis=0, concat_axis=0, tiled=True)


def groups_of(count):
    if count < 4:
        return [[step] for step in range(count)]
    middle = list(range(1, count))
    middle.remove(count // 2)
    return [[0], middle, [count // 2]]


def exchange_body(band_size, fft_size, orbitals, partners, shift_table, shift_index):
    extent = orbitals.shape[2]
    band_count, slab = orbitals.shape[:2]
    partner_count = partners.shape[0]
    row_count = extent // 2 // fft_size
    my_band = lax.axis_index("band")
    row_start = lax.axis_index("fft") * row_count
    forward_tables = stage_tables(extent, -1.0)
    inverse_tables = stage_tables(extent, 1.0)

    arrived = [partners] + [
        ring_shift(partners, "band", band_size, step) for step in range(1, band_size)
    ]
    potential = None
    for steps in groups_of(band_size):
        block = jnp.concatenate([arrived[step] for step in steps], axis=0)
        ids = jnp.concatenate(
            [
                (my_band - step) % band_size * partner_count + jnp.arange(partner_count)
                for step in steps
            ]
        )
        first, plane = kernel_parts(
            shift_table[shift_index[ids]], row_start, row_count, extent
        )
        spectrum = forward_call(orbitals, block, forward_tables, fft_size)
        spectrum = lax.all_to_all(spectrum, "fft", split_axis=0, concat_axis=0, tiled=True)
        spectrum = middle_call(first, plane, spectrum)
        spectrum = lax.all_to_all(spectrum, "fft", split_axis=0, concat_axis=0, tiled=True)
        potential = inverse_call(spectrum, block, potential, inverse_tables)

    def spread(value):
        rows = value.reshape(band_count, band_size, -1, 2 * extent).swapaxes(0, 1)
        rows = lax.all_to_all(rows, "band", split_axis=0, concat_axis=0, tiled=True)
        return rows.reshape(band_count * band_size, -1, 2 * extent)

    sub_orbitals = spread(orbitals)
    sub_pot = spread(potential)
    total_bands = sub_pot.shape[0]
    sub_turned = rotate(sub_pot)
    flat_pot = sub_pot.reshape(total_bands, -1)
    flat_turned = sub_turned.reshape(total_bands, -1)
    both = jnp.stack([flat_pot, flat_turned])
    over = jnp.einsum("ik,cjk->cij", sub_orbitals.reshape(total_bands, -1), both, precision=PREC)
    size = max(8, total_bands)
    over = jnp.pad(over, ((0, 0), (0, size - total_bands), (0, size - total_bands)))
    pieces = gather_small(over, ("band", "fft"), band_size * fft_size)
    inverse = factor_inverse(pieces, total_bands, 1.0 / float(extent**3))
    inverse = inverse[:, :total_bands, :total_bands]
    projector = jnp.einsum("clm,cmk->lk", inverse, both, precision=PREC)
    projector = projector.reshape(band_size, band_count, -1, 2 * extent)
    projector = lax.all_to_all(projector, "band", split_axis=0, concat_axis=0, tiled=True)
    return (potential, projector.swapaxes(0, 1).reshape(orbitals.shape))


def solution(mesh):
    spec = P(("kgrp", "band"), "fft", None, None)
    band_size, fft_size = mesh.shape["band"], mesh.shape["fft"]
    body = lambda *arrays: exchange_body(band_size, fft_size, *arrays)
    return jax.shard_map(
        body,
        mesh=mesh,
        in_specs=(spec, spec, P(), P("kgrp")),
        out_specs=(spec, spec),
        check_vma=False,
    )
```

```python
import math

import jax
import jax.numpy as jnp
import numpy as np
from jax import lax
from jax.experimental import pallas as pl
from jax.experimental.pallas import tpu as pltpu
from jax.sharding import PartitionSpec as P


PREC = lax.Precision.HIGH
SCREEN_SQUARE = 0.25
FOUR_PI = 4.0 * math.pi


def lane_table(extent, sign):
    index = np.arange(extent)
    wave = np.exp(sign * 2j * np.pi / extent * (np.outer(index, index) % extent))
    full = np.kron(np.array([[1.0, 1.0], [1.0, -1.0]]), wave)
    return np.block([[full.real, full.imag], [-full.imag, full.real]])


def row_table(half, sign):
    index = np.arange(half)
    wave = np.exp(sign * 2j * np.pi / half * (np.outer(index, index) % half))
    return np.block([[wave.real, -wave.imag], [wave.imag, wave.real]])


def twiddle_table(extent, sign):
    half = extent // 2
    wave = np.exp(sign * 2j * np.pi / extent * np.arange(half))
    wave = np.concatenate(
        [np.ones((half, extent)), np.broadcast_to(wave[:, None], (half, extent))], axis=1
    )
    return jnp.asarray(np.stack([wave.real, wave.imag]), jnp.float32)


def halves(table):
    table = np.asarray(table, np.float32)
    high = table.astype(jnp.bfloat16)
    low = (table - high.astype(np.float32)).astype(jnp.bfloat16)
    return high, low


def stage_tables(extent, sign):
    high, low = halves(lane_table(extent, sign))
    lanes = jnp.stack([jnp.asarray(high), jnp.asarray(low)])
    high, low = halves(row_table(extent // 2, sign))
    rows = jnp.asarray(np.concatenate([high, high, low], axis=1))
    return lanes, rows, twiddle_table(extent, sign)


def split_value(value):
    high = value.astype(jnp.bfloat16)
    low = (value - high.astype(jnp.float32)).astype(jnp.bfloat16)
    return high, low


def dot(left, right):
    return jnp.dot(left, right, preferred_element_type=jnp.float32)


def on_lanes(real, imag, table_ref):
    high, low = split_value(jnp.concatenate([real, imag], axis=1))
    out = dot(high, table_ref[0]) + (dot(low, table_ref[0]) + dot(high, table_ref[1]))
    lanes = real.shape[1]
    return out[:, :lanes], out[:, lanes:]


def on_rows(stacked, table_ref):
    high, low = split_value(stacked)
    return dot(table_ref[...], jnp.concatenate([high, low, high], axis=0))


def unpack(tile):
    half, extent = tile.shape[0] // 2, tile.shape[1] // 2
    top, bottom = tile[:half], tile[half:]
    first = lax.broadcasted_iota(jnp.int32, top.shape, 1) < extent
    real = jnp.where(first, top, pltpu.roll(bottom, extent, 1))
    imag = jnp.where(first, pltpu.roll(top, extent, 1), bottom)
    return real, imag


def pack(real, imag):
    extent = real.shape[1] // 2
    first = lax.broadcasted_iota(jnp.int32, real.shape, 1) < extent
    top = jnp.where(first, real, pltpu.roll(imag, extent, 1))
    bottom = jnp.where(first, pltpu.roll(real, extent, 1), imag)
    return top, bottom


def forward_kernel(orb_ref, part_ref, lanes_ref, rows_ref, twid_ref, out_ref):
    count, extent = orb_ref.shape[1], orb_ref.shape[2]
    half = extent // 2
    devices, share = out_ref.shape[0], out_ref.shape[5]
    reals, imags = [], []
    for x in range(count):
        orb_real, orb_imag = unpack(orb_ref[0, x])
        part_real, part_imag = unpack(part_ref[0, x])
        reals.append(part_real * orb_real + part_imag * orb_imag)
        imags.append(part_real * orb_imag - part_imag * orb_real)
    real, imag = on_lanes(jnp.concatenate(reals, 0), jnp.concatenate(imags, 0), lanes_ref)
    cosine, sine = twid_ref[0], twid_ref[1]
    for x in range(0, count, 2):
        pair = []
        for at in (x, x + 1):
            re, im = real[at * half : (at + 1) * half], imag[at * half : (at + 1) * half]
            pair.append(
                jnp.concatenate([re * cosine - im * sine, re * sine + im * cosine], axis=0)
            )
        done = on_rows(jnp.concatenate(pair, axis=1), rows_ref)
        for at in (0, 1):
            piece = done[:, at * 2 * extent : (at + 1) * 2 * extent]
            for device in range(devices):
                lo = device * share
                out_ref[device, 0, 0, 0, x + at] = piece[lo : lo + share]
                out_ref[device, 0, 0, 1, x + at] = piece[half + lo : half + lo + share]


def inverse_kernel(spec_ref, part_ref, *refs, chained):
    prior_ref = refs[0] if chained else None
    lanes_ref, rows_ref, twid_ref, out_ref = refs[-4:]
    count, extent = part_ref.shape[1], part_ref.shape[2]
    half = extent // 2
    devices = spec_ref.shape[0]
    cosine, sine = twid_ref[0], twid_ref[1]
    reals, imags = [], []
    for x in range(0, count, 2):
        stacked = jnp.concatenate(
            [
                jnp.concatenate(
                    [spec_ref[d, 0, 0, c, at] for c in (0, 1) for d in range(devices)], axis=0
                )
                for at in (x, x + 1)
            ],
            axis=1,
        )
        done = on_rows(stacked, rows_ref)
        for at in (0, 1):
            piece = done[:, at * 2 * extent : (at + 1) * 2 * extent]
            re, im = piece[:half], piece[half:]
            reals.append(re * cosine - im * sine)
            imags.append(re * sine + im * cosine)
    real, imag = on_lanes(jnp.concatenate(reals, 0), jnp.concatenate(imags, 0), lanes_ref)
    first = pl.program_id(2) == 0
    for x in range(count):
        re, im = real[x * half : (x + 1) * half], imag[x * half : (x + 1) * half]
        part_real, part_imag = unpack(part_ref[0, x])
        top, bottom = pack(part_real * re - part_imag * im, part_real * im + part_imag * re)
        value = jnp.concatenate([top, bottom], axis=0)
        before = prior_ref[0, x] if chained else jnp.zeros_like(value)
        out_ref[0, x] = value + jnp.where(first, before, out_ref[0, x])


def turn(real, imag, step, count, sign):
    step = step % count
    if step == 0:
        return real, imag
    if 4 * step == count:
        return (-imag, real) if sign > 0 else (imag, -real)
    if 2 * step == count:
        return -real, -imag
    if 4 * step == 3 * count:
        return (imag, -real) if sign > 0 else (-imag, real)
    angle = 2.0 * math.pi * step / count
    cosine, sine = math.cos(angle), sign * math.sin(angle)
    return real * cosine - imag * sine, real * sine + imag * cosine


def small_dft(values, sign):
    count = len(values)
    if count == 1:
        return values
    even, odd = small_dft(values[0::2], sign), small_dft(values[1::2], sign)
    low, high = [], []
    for step in range(count // 2):
        turned_real, turned_imag = turn(*odd[step], step, count, sign)
        low.append((even[step][0] + turned_real, even[step][1] + turned_imag))
        high.append((even[step][0] - turned_real, even[step][1] - turned_imag))
    return low + high


def long_dft(values, sign):
    count, first = len(values), 1
    while first * first < count:
        first *= 2
    second = count // first
    columns = []
    for offset in range(second):
        part = small_dft(values[offset::second], sign)
        columns.append([turn(*part[k], offset * k, count, sign) for k in range(first)])
    out = [None] * count
    for k in range(first):
        for block, value in enumerate(small_dft([column[k] for column in columns], sign)):
            out[k + first * block] = value
    return out


def middle_kernel(first_ref, plane_ref, spec_ref, out_ref, *, start):
    field = pl.program_id(1) + start
    devices, slab = spec_ref.shape[0], spec_ref.shape[4]
    extent = devices * slab
    plane = plane_ref[0]
    values = [
        (spec_ref[x // slab, 0, 0, 0, x % slab], spec_ref[x // slab, 0, 0, 1, x % slab])
        for x in range(extent)
    ]
    values = long_dft(values, -1.0)
    scale = FOUR_PI / extent**3
    scaled = []
    for x, (real, imag) in enumerate(values):
        kernel = scale / (first_ref[field, x] + plane)
        scaled.append((real * kernel, imag * kernel))
    for x, (real, imag) in enumerate(long_dft(scaled, 1.0)):
        out_ref[x // slab, 0, 0, 0, x % slab] = real
        out_ref[x // slab, 0, 0, 1, x % slab] = imag


def whole_block(array):
    return pl.BlockSpec(array.shape, lambda *_: (0,) * array.ndim)


def chunk_of(slab):
    return math.gcd(slab, 8)


def cost(flops, count):
    return pl.CostEstimate(flops=int(flops), bytes_accessed=int(count), transcendentals=0)


def forward_call(orbitals, block, tables, devices):
    bands, slab, extent, lanes = orbitals.shape
    fields, step = block.shape[0], chunk_of(orbitals.shape[1])
    share = extent // 2 // devices
    grid_block = (1, step, extent, lanes)
    return pl.pallas_call(
        forward_kernel,
        grid=(bands, fields, slab // step),
        in_specs=[
            pl.BlockSpec(grid_block, lambda i, j, x: (i, x, 0, 0)),
            pl.BlockSpec(grid_block, lambda i, j, x: (j, x, 0, 0)),
        ]
        + [whole_block(table) for table in tables],
        out_specs=pl.BlockSpec(
            (devices, 1, 1, 2, step, share, lanes), lambda i, j, x: (0, i, j, 0, x, 0, 0)
        ),
        out_shape=jax.ShapeDtypeStruct(
            (devices, bands, fields, 2, slab, share, lanes), jnp.float32
        ),
        cost_estimate=cost(bands * fields * 1e9, bands * fields * orbitals[0].size * 12),
        name="forward",
    )(orbitals, block, *tables)


def middle_call(first_part, plane, start, spectrum):
    devices, bands, fields, _, slab, share, lanes = spectrum.shape
    spec = pl.BlockSpec(
        (devices, 1, 1, 2, slab, share, lanes), lambda i, j: (0, i, j, 0, 0, 0, 0)
    )
    body = lambda *refs: middle_kernel(*refs, start=start)
    return pl.pallas_call(
        body,
        grid=(bands, fields),
        in_specs=[
            pl.BlockSpec(memory_space=pltpu.SMEM),
            pl.BlockSpec((1, share, lanes), lambda i, j: (j + start, 0, 0)),
            spec,
        ],
        out_specs=spec,
        out_shape=jax.ShapeDtypeStruct(spectrum.shape, jnp.float32),
        cost_estimate=cost(bands * fields * 1e9, spectrum.size * 8),
        name="middle",
    )(first_part, plane, spectrum)


def inverse_call(spectrum, block, prior, tables):
    devices, bands, fields, _, slab, share, lanes = spectrum.shape
    extent, step = block.shape[2], chunk_of(slab)
    grid_block = (1, step, extent, lanes)
    by_band = pl.BlockSpec(grid_block, lambda i, x, j: (i, x, 0, 0))
    chained = prior is not None
    extra = [prior] if chained else []
    body = lambda *refs: inverse_kernel(*refs, chained=chained)
    return pl.pallas_call(
        body,
        grid=(bands, slab // step, fields),
        in_specs=[
            pl.BlockSpec(
                (devices, 1, 1, 2, step, share, lanes), lambda i, x, j: (0, i, j, 0, x, 0, 0)
            ),
            pl.BlockSpec(grid_block, lambda i, x, j: (j, x, 0, 0)),
        ]
        + [by_band] * len(extra)
        + [whole_block(table) for table in tables],
        out_specs=by_band,
        out_shape=jax.ShapeDtypeStruct((bands, slab, extent, lanes), jnp.float32),
        cost_estimate=cost(bands * fields * 1e9, bands * fields * block[0].size * 12),
        name="inverse",
    )(spectrum, block, *extra, *tables)


def rotate(field):
    extent = field.shape[-1] // 2
    return jnp.concatenate([field[..., extent:], -field[..., :extent]], axis=-1)


def frequency(positions, extent):
    return jnp.where(positions < extent // 2, positions, positions - extent).astype(jnp.float32)


def kernel_parts(qvectors, row_start, row_count, extent):
    index = jnp.arange(extent, dtype=jnp.int32)
    parity = jnp.arange(2, dtype=jnp.int32)
    ky = 2 * (row_start + jnp.arange(row_count, dtype=jnp.int32))[:, None] + parity
    first = (frequency(index, extent)[None, :] + qvectors[:, 0:1]) ** 2
    second = (frequency(ky, extent)[None] + qvectors[:, 1, None, None]) ** 2
    third = (frequency(index, extent)[None, :] + qvectors[:, 2:3]) ** 2
    plane = second[:, :, :, None] + third[:, None, None, :] + SCREEN_SQUARE
    return first, plane.reshape(qvectors.shape[0], row_count, 2 * extent)


def factor_kernel(over_ref, inv_ref, *, order, scale):
    total = jnp.sum(over_ref[...], axis=0) * scale
    size = total.shape[-1]
    res_real, res_imag = total[0], total[1]
    rows = lax.broadcasted_iota(jnp.int32, (size, size), 0)
    cols = lax.broadcasted_iota(jnp.int32, (size, size), 1)
    same = rows == cols
    inv_real = jnp.where(same, 1.0, 0.0).astype(jnp.float32)
    inv_imag = jnp.zeros_like(inv_real)
    across = lambda v: jnp.sum(v, axis=1, keepdims=True)
    down = lambda v: jnp.sum(v, axis=0, keepdims=True)
    for step in range(order):
        at_col = cols == step
        pivot = down(across(jnp.where(at_col & (rows == step), res_real, 0.0)))
        root = 1.0 / jnp.sqrt(pivot)
        below = at_col & (rows > step)
        col_real = across(jnp.where(below, res_real, 0.0)) * root
        col_imag = across(jnp.where(below, res_imag, 0.0)) * root
        row_real = down(jnp.where(same, col_real, 0.0))
        row_imag = down(jnp.where(same, col_imag, 0.0))
        res_real = res_real - (col_real * row_real + col_imag * row_imag)
        res_imag = res_imag - (col_imag * row_real - col_real * row_imag)
        at_row = rows == step
        inv_real = jnp.where(at_row, inv_real * root, inv_real)
        inv_imag = jnp.where(at_row, inv_imag * root, inv_imag)
        lead_real = down(jnp.where(at_row, inv_real, 0.0))
        lead_imag = down(jnp.where(at_row, inv_imag, 0.0))
        inv_real = inv_real - (col_real * lead_real - col_imag * lead_imag)
        inv_imag = inv_imag - (col_real * lead_imag + col_imag * lead_real)
    inv_ref[0] = inv_real
    inv_ref[1] = inv_imag


def factor_inverse(pieces, order, scale):
    size = pieces.shape[-1]
    body = lambda a, b: factor_kernel(a, b, order=order, scale=scale)
    return pl.pallas_call(
        body, out_shape=jax.ShapeDtypeStruct((2, size, size), jnp.float32), name="factor"
    )(pieces)


def gather_small(value, axis_name, count):
    copies = jnp.broadcast_to(value[None], (count,) + value.shape)
    return lax.all_to_all(copies, axis_name, split_axis=0, concat_axis=0, tiled=True)


def source_of(place, step, count):
    return place ^ step if count & (count - 1) == 0 else (place - step) % count


def fetch(value, step, count):
    pairs = [(source_of(place, step, count), place) for place in range(count)]
    return lax.ppermute(value, "band", pairs)


def after(value, earlier):
    return lax.optimization_barrier((value, earlier))[0]


def exchange_body(band_size, fft_size, orbitals, partners, shift_table, shift_index):
    extent = orbitals.shape[2]
    band_count, _ = orbitals.shape[:2]
    partner_count = partners.shape[0]
    row_count = extent // 2 // fft_size
    my_band = lax.axis_index("band")
    row_start = lax.axis_index("fft") * row_count
    forward_tables = stage_tables(extent, -1.0)
    inverse_tables = stage_tables(extent, 1.0)

    def spread(value):
        rows = value.reshape(band_count, band_size, -1, 2 * extent).swapaxes(0, 1)
        rows = lax.all_to_all(rows, "band", split_axis=0, concat_axis=0, tiled=True)
        return rows.reshape(band_count * band_size, -1, 2 * extent)

    arrived, ids = [partners], []
    for step in range(1, band_size):
        source = after(partners, arrived[-1]) if step > 2 else partners
        arrived.append(fetch(source, step, band_size))
    for step in range(band_size):
        owner = source_of(my_band, step, band_size)
        ids.append(owner * partner_count + jnp.arange(partner_count))
    qvectors = shift_table[shift_index[jnp.concatenate(ids)]]
    first, plane = kernel_parts(qvectors, row_start, row_count, extent)

    spectra, middles, potential, done = [], [], None, 0

    def finish(potential):
        return inverse_call(spectra[done], arrived[done], potential, inverse_tables)

    for step in range(band_size):
        block = arrived[step]
        if step >= 1:
            block = after(block, middles[-1])
        if step >= 2:
            potential = finish(potential)
            done += 1
            block = after(block, potential)
        sent = forward_call(orbitals, block, forward_tables, fft_size)
        spectrum = lax.all_to_all(sent, "fft", split_axis=0, concat_axis=0, tiled=True)
        spectrum = middle_call(first, plane, step * partner_count, spectrum)
        middles.append(spectrum)
        if step == band_size - 1:
            sub_orbitals = spread(after(orbitals, sent))
            spectrum = after(spectrum, sub_orbitals)
        spectrum = lax.all_to_all(spectrum, "fft", split_axis=0, concat_axis=0, tiled=True)
        spectra.append(spectrum)
    while done < band_size:
        potential = finish(potential)
        done += 1

    sub_pot = spread(potential)
    total_bands = sub_pot.shape[0]
    sub_turned = rotate(sub_pot)
    flat_pot = sub_pot.reshape(total_bands, -1)
    flat_turned = sub_turned.reshape(total_bands, -1)
    both = jnp.stack([flat_pot, flat_turned])
    over = jnp.einsum("ik,cjk->cij", sub_orbitals.reshape(total_bands, -1), both, precision=PREC)
    size = max(8, total_bands)
    over = jnp.pad(over, ((0, 0), (0, size - total_bands), (0, size - total_bands)))
    pieces = gather_small(over, ("band", "fft"), band_size * fft_size)
    inverse = factor_inverse(pieces, total_bands, 1.0 / float(extent**3))
    inverse = inverse[:, :total_bands, :total_bands]
    projector = jnp.einsum("clm,cmk->lk", inverse, both, precision=PREC)
    projector = projector.reshape(band_size, band_count, -1, 2 * extent)
    projector = lax.all_to_all(projector, "band", split_axis=0, concat_axis=0, tiled=True)
    return (potential, projector.swapaxes(0, 1).reshape(orbitals.shape))


def solution(mesh):
    spec = P(("kgrp", "band"), "fft", None, None)
    band_size, fft_size = mesh.shape["band"], mesh.shape["fft"]

    def body(*arrays):
        return exchange_body(band_size, fft_size, *arrays)

    return jax.shard_map(
        body,
        mesh=mesh,
        in_specs=(spec, spec, P(), P("kgrp")),
        out_specs=(spec, spec),
        check_vma=False,
    )
```
